32 devices in a mesh: rows: 2 (over core), cols: 4 (over y, x), slabs: 4 (over z).
Axes of the slice: x: 2, y: 2, z: 4, core: 2. Of those that a mesh axis runs over, the one named last changes fastest.
Arguments:
- tracer: float32 [8, 256, 384, 128], P('rows', 'cols', 'slabs'), may hold values from 0.2 to 1.8
- crowding: float32 [8, 256, 384, 128], P('rows', 'cols', 'slabs'), may hold values from 0.5 to 2
Outputs:
- tracer_end: float32 [8, 256, 384, 128], P('rows', 'cols', 'slabs')
The draws below stay inside these ranges and needn't reach their ends.
All inputs are finite; a program needn't handle non-finite values.
Results may differ from the reference program's by a relative error of at most 0.00002.
Values sent between devices are 32-bit elements.
No kernel may reach another device: no remote copies, remote signals or barrier semaphores. Data moves between devices by JAX's collectives and lax.ppermute only.
A program may use at most 448 MiB of HBM per device.

```python
import jax
import jax.numpy as jnp
from jax import lax

GRID_Y = 8
GRID_X = 256
GRID_Z = 384
SPECIES = 128
STEPS = 4


def block_levels(key, shape, cuts, smallest, top_value):
    loudness = 1.0
    for dim, shards_of in cuts:
        steps = jax.random.uniform(jax.random.fold_in(jax.random.fold_in(key, 6), dim), (shards_of,), jnp.float32, smallest / len(cuts), top_value / len(cuts))
        loudness = loudness * jnp.repeat(jnp.exp(steps), shape[dim] // shards_of).reshape((-1,) + (1,) * (len(shape) - 1 - dim))
    return loudness


def setup_inputs(seed: int = 0) -> dict:
    key_of = jax.random.split(jax.random.key(seed), 3)
    return {
        "tracer": jnp.clip(0.2 + 1.5999999 * jax.random.uniform(key_of[0], (GRID_Y, GRID_X, GRID_Z, SPECIES), jnp.float32) ** block_levels(key_of[0], (GRID_Y, GRID_X, GRID_Z, SPECIES), ((0, 2), (1, 4), (2, 4)), -0.2, 0.2), 0.2, 1.8),
        "crowding": jnp.clip(0.5 + 1.5 * jax.random.uniform(key_of[1], (GRID_Y, GRID_X, GRID_Z, SPECIES), jnp.float32) ** block_levels(key_of[1], (GRID_Y, GRID_X, GRID_Z, SPECIES), ((0, 2), (1, 4), (2, 4)), -0.2, 0.2), 0.5, 2.0),
    }


def inner_cells(values, dims):
    for dim in dims:
        values = lax.slice_in_dim(values, 1, values.shape[dim] - 1, axis=dim)
    return values


def side_cells(values, dim, start, dims):
    others = [other for other in dims if other != dim]
    values = inner_cells(values, others)
    return lax.slice_in_dim(values, start, start + values.shape[dim] - 2, axis=dim)


def advance(padded, crowding):
    middle = inner_cells(padded, (0, 1, 2))
    lower = [side_cells(padded, dim, 0, (0, 1, 2)) for dim in (0, 1, 2)]
    upper = [side_cells(padded, dim, 2, (0, 1, 2)) for dim in (0, 1, 2)]
    spread = lower[0] + upper[0] + lower[1] + upper[1] + lower[2] + upper[2] - 6.0 * middle
    return middle + 0.1 * spread + 0.2 * middle * (1.0 - middle * crowding)


def reference(tracer, crowding):
    for step in range(STEPS):
        tracer = advance(jnp.pad(tracer, ((1, 1), (1, 1), (1, 1), (0, 0)), mode="constant"), crowding)
    return tracer
```

```python
import functools

import jax
import jax.numpy as jnp
from jax import lax
from jax.experimental import pallas as pl
from jax.experimental.pallas import tpu as pltpu
from jax.sharding import PartitionSpec as P

STEPS = 4
SUB = 8
VMEM_SPEC = pl.BlockSpec(memory_space=pltpu.VMEM)
HBM_SPEC = pl.BlockSpec(memory_space=pltpu.HBM)


def matchings(count):
    swaps = []
    for first in (0, 1):
        pairs = [(i, i + 1) for i in range(first, count - 1, 2)]
        if pairs:
            swaps.append(pairs + [(b, a) for a, b in pairs])
    return swaps


def swap(face, axis, which, count):
    with jax.named_scope(f"swap_{axis}_{which}"):
        return lax.ppermute(face, axis, matchings(count)[which])


def near(which, parity, size):
    high = parity == which
    return jnp.where(high, size - 1, 0)


def mirrored(j, parity, rows):
    return jnp.where(parity == 0, j, rows - 1 - j)


def pack_kernel(dims, counts, tracer, *refs):
    rows, nx, nz = dims
    n_y, n_x, n_z = counts
    faces, (groups, sems) = refs[: sum(counts)], refs[sum(counts) :]
    y_faces, x_faces, z_faces = faces[:n_y], faces[n_y : n_y + n_x], faces[n_y + n_x :]
    py = lax.rem(lax.axis_index("rows"), 2)
    px = lax.rem(lax.axis_index("cols"), 2)
    pz = lax.rem(lax.axis_index("slabs"), 2)
    order = [mirrored(j, py, rows) for j in range(rows)]
    z_copies, copies = [], []
    for which in range(n_z):
        z = pl.multiple_of(near(which, pz, nz // SUB) * SUB, SUB)
        for j in range(rows):
            z_copies.append((tracer.at[order[j], :, pl.ds(z, SUB), :], groups.at[which, j]))
    for which in range(n_x):
        for j in range(rows):
            copies.append((tracer.at[order[j], near(which, px, nx)], x_faces[which].at[j]))
    for which in range(n_y):
        copies.append((tracer.at[order[rows - 1 if which == 0 else 0]], y_faces[which]))
    started = []
    for k, (src, dst) in enumerate(z_copies + copies):
        copy = pltpu.make_async_copy(src, dst, sems.at[k])
        copy.start()
        started.append(copy)
    for copy in started[: len(z_copies)]:
        copy.wait()
    for which in range(n_z):
        z = near(which, pz, SUB)
        for j in range(rows):
            cells = groups.at[which, j].reshape(nx * SUB, 128)
            for x in range(0, nx, SUB):
                face = cells[pl.ds(x * SUB + z, SUB, stride=SUB), :]
                z_faces[which][j, pl.ds(x, SUB), :] = face
    for copy in started[len(z_copies) :]:
        copy.wait()


def bulk_kernel(dims, counts, step, pitches, *refs):
    rows, nx, nz = dims
    first, last = step == 0, step == STEPS - 1
    src, refs = (refs[:1], refs[1:]) if first else (refs[:rows], refs[rows:])
    halos, refs = refs[: counts[0]], refs[counts[0] :]
    crowding, outs = refs[0], refs[1:]
    py = lax.rem(lax.axis_index("rows"), 2)
    order = [mirrored(j, py, rows) for j in range(rows)]
    pitch = nz + 1

    if not last:
        zero = jnp.zeros((SUB, 128), jnp.float32)
        for out in outs:
            for x in range(0, nx, SUB):
                out[pl.ds(x * pitch, SUB, stride=pitch), :] = zero
            out[pl.ds(nx * pitch, SUB), :] = zero

    scale = 2.0 * 10.0**-step

    def column(z, edge):
        def load(j, x, shift):
            if first:
                ref = src[0].at[order[j]]
                if shift == 0:
                    return ref[x, pl.ds(z, SUB), :]
                if edge == shift:
                    own = ref[x, pl.ds(z, SUB), :]
                    rolled = pltpu.roll(own, (-shift) % SUB, 0)
                    row = lax.broadcasted_iota(jnp.int32, (SUB, 128), 0)
                    return jnp.where(row == (0 if shift < 0 else SUB - 1), 0.0, rolled)
                return ref[x, pl.ds(z + shift, SUB), :]
            return src[j][pl.ds(x * pitch + 1 + z + shift, SUB), :]

        def load_halo(which, x):
            if first:
                return halos[which][x, pl.ds(z, SUB), :]
            return halos[which][pl.ds(x * pitch + 1 + z, SUB), :]

        def plane(x):
            cells = [load(j, x, 0) for j in range(rows)]
            cells.append(load_halo(0, x))
            below = load_halo(1, x) if counts[0] > 1 else None
            return cells, below

        def advance(x, carry, final):
            diag, here, below = carry
            if final:
                after, after_below = None, None
            else:
                after, after_below = plane(x + 1)
            forward = []
            for j in range(-1, rows):
                own = below if j < 0 else here[j]
                if final:
                    forward.append(own)
                elif own is None:
                    forward.append(after[j + 1])
                else:
                    forward.append(own + after[j + 1])
            for j in range(rows):
                total = load(j, x, -1) + load(j, x, 1)
                total = total + diag[j]
                if forward[j] is not None:
                    total = total + forward[j]
                cell = here[j]
                c = crowding[order[j], x, pl.ds(z, SUB), :]
                value = total + cell * (6.0 - (c * scale) * cell)
                if last:
                    outs[0][order[j], x, pl.ds(z, SUB), :] = value * 10.0**-STEPS
                else:
                    outs[j][pl.ds(x * pitch + 1 + z, SUB), :] = value
            return forward[1:], after[:rows] if after else None, after_below

        start, start_below = plane(0)
        carry = (start[1:], start[:rows], start_below)
        unroll = 3 if (nx - 1) % 3 == 0 else 1

        def body(i, carry):
            for k in range(unroll):
                carry = advance(i * unroll + k, carry, False)
            return carry

        carry = lax.fori_loop(0, (nx - 1) // unroll, body, carry)
        advance(nx - 1, carry, True)

    groups = nz // SUB
    if first:
        column(0, -1)
        pl.loop(1, groups - 1)(lambda g: column(pl.multiple_of(g * SUB, SUB), 0))
        column(nz - SUB, 1)
    else:
        pl.loop(0, groups)(lambda g: column(pl.multiple_of(g * SUB, SUB), 0))


def patch_kernel(dims, counts, step, *refs):
    rows, nx, nz = dims
    last = step == STEPS - 1
    n_state = 1 if last else rows
    state, refs = refs[:n_state], refs[n_state:]
    n_x, n_z = counts[1], counts[2]
    halo_x, halo_z, refs = refs[:n_x], refs[n_x : n_x + n_z], refs[n_x + n_z :]
    out, refs = refs[:n_state], refs[n_state:]
    face_x, face_z = (None, None) if last else (refs[:n_x], refs[n_x : n_x + n_z])
    py = lax.rem(lax.axis_index("rows"), 2)
    px = lax.rem(lax.axis_index("cols"), 2)
    pz = lax.rem(lax.axis_index("slabs"), 2)
    pitch = nz if last else nz + 1
    offset = 0 if last else 1

    def view(refs, j):
        return refs[0].at[mirrored(j, py, rows)] if last else refs[j]

    def scaled(values):
        return values * 10.0**-STEPS if last else values

    for which in range(n_z):
        z = near(which, pz, nz)
        for j in range(rows):
            for x in range(0, nx, SUB):
                at = (pl.ds(x * pitch + offset + z, SUB, stride=pitch), slice(None))
                view(out, j)[at] = view(out, j)[at] + scaled(halo_z[which][j, pl.ds(x, SUB), :])
    for which in range(n_x):
        x = near(which, px, nx)
        for j in range(rows):
            for z in range(0, nz, SUB):
                at = (pl.ds(x * pitch + offset + z, SUB), slice(None))
                value = view(out, j)[at] + scaled(halo_x[which][j, pl.ds(z, SUB), :])
                view(out, j)[at] = value
                if not last:
                    face_x[which][j, pl.ds(z, SUB), :] = value
    if not last:
        for which in range(n_z):
            z = near(which, pz, nz)
            for j in range(rows):
                for x in range(0, nx, SUB):
                    at = (pl.ds(x * pitch + offset + z, SUB, stride=pitch), slice(None))
                    face_z[which][j, pl.ds(x, SUB), :] = out[j][at]


def call(kernel, name, out_shape, args, out_specs=None, in_specs=None, aliases=None, scratch=(), vmem=1):
    return pl.pallas_call(
        kernel,
        name=name,
        out_shape=out_shape,
        in_specs=in_specs or [VMEM_SPEC] * len(args),
        out_specs=out_specs or [VMEM_SPEC] * len(out_shape),
        input_output_aliases=aliases or {},
        scratch_shapes=list(scratch),
        compiler_params=pltpu.CompilerParams(vmem_limit_bytes=vmem * 1024 * 1024),
    )(*args)


def on_device(tracer, crowding):
    rows, nx, nz, species = tracer.shape
    dims = (rows, nx, nz)
    sizes = [lax.axis_size(axis) for axis in ("rows", "cols", "slabs")]
    counts = [len(matchings(size)) for size in sizes]
    pitch_rows = -(-(nx * (nz + 1) + SUB) // SUB) * SUB
    f32 = jnp.float32
    full_row = pltpu.VMEM((nx, nz, species), f32)
    state_row = pltpu.VMEM((pitch_rows, species), f32)
    x_face = pltpu.VMEM((rows, nz, species), f32)
    z_face = pltpu.VMEM((rows, nx, species), f32)

    out_shape = [full_row] * counts[0] + [x_face] * counts[1] + [z_face] * counts[2]
    packed = call(
        functools.partial(pack_kernel, dims, counts),
        "pack",
        out_shape,
        (pltpu.with_memory_space_constraint(tracer, pltpu.HBM),),
        in_specs=[HBM_SPEC],
        scratch=[
            pltpu.VMEM((counts[2], rows, nx, SUB, species), f32),
            pltpu.SemaphoreType.DMA((counts[0] + rows * (counts[1] + counts[2]),)),
        ],
        vmem=4,
    )
    y_faces, packed = packed[: counts[0]], packed[counts[0] :]
    x_faces, z_faces = packed[: counts[1]], packed[counts[1] :]
    state = [tracer]
    for step in range(STEPS):
        last = step == STEPS - 1
        y_halos = [swap(face, "rows", k, sizes[0]) for k, face in enumerate(y_faces)]
        x_halos = [swap(face, "cols", k, sizes[1]) for k, face in enumerate(x_faces)]
        z_halos = [swap(face, "slabs", k, sizes[2]) for k, face in enumerate(z_faces)]
        if last:
            out_shape = [pltpu.VMEM(tracer.shape, f32)]
        else:
            out_shape = [state_row] * rows
        state = call(
            functools.partial(bulk_kernel, dims, counts, step, None),
            f"bulk{step}",
            out_shape,
            (*state, *y_halos, crowding),
        )
        args = (*state, *x_halos, *z_halos)
        if last:
            out_shape = [pltpu.VMEM((rows, nx * nz, species), f32)]
            args = (state[0].reshape(rows, nx * nz, species), *args[1:])
        else:
            out_shape = [state_row] * rows + [x_face] * counts[1] + [z_face] * counts[2]
        patched = call(
            functools.partial(patch_kernel, dims, counts, step),
            f"patch{step}",
            out_shape,
            args,
            aliases={k: k for k in range(len(state))},
        )
        if not last:
            state = patched[:rows]
            y_faces = [state[rows - 1 if k == 0 else 0] for k in range(counts[0])]
            x_faces = patched[rows : rows + counts[1]]
            z_faces = patched[rows + counts[1] :]
    return patched[0].reshape(rows, nx, nz, species)


def solution(mesh):
    placed = (P("rows", "cols", "slabs", None), P("rows", "cols", "slabs", None))
    return jax.shard_map(
        on_device,
        mesh=mesh,
        in_specs=placed,
        out_specs=P("rows", "cols", "slabs", None),
        check_vma=False,
    )
```

```python
import functools

import jax
import jax.numpy as jnp
from jax import lax
from jax.experimental import pallas as pl
from jax.experimental.pallas import tpu as pltpu
from jax.sharding import PartitionSpec as P

STEPS = 4
SUB = 8
VMEM_SPEC = pl.BlockSpec(memory_space=pltpu.VMEM)
HBM_SPEC = pl.BlockSpec(memory_space=pltpu.HBM)


def matchings(count):
    swaps = []
    for first in (0, 1):
        pairs = [(i, i + 1) for i in range(first, count - 1, 2)]
        if pairs:
            swaps.append(pairs + [(b, a) for a, b in pairs])
    return swaps


def swap(face, axis, which, count):
    with jax.named_scope(f"swap_{axis}_{which}"):
        return lax.ppermute(face, axis, matchings(count)[which])


def near(which, parity, size):
    high = parity == which
    return jnp.where(high, size - 1, 0)


def mirrored(j, parity, rows):
    return jnp.where(parity == 0, j, rows - 1 - j)


def pack_kernel(dims, counts, tracer, *refs):
    rows, nx, nz = dims
    n_y, n_x, n_z = counts
    faces, (groups, sems) = refs[: sum(counts)], refs[sum(counts) :]
    y_faces, x_faces, z_faces = faces[:n_y], faces[n_y : n_y + n_x], faces[n_y + n_x :]
    py = lax.rem(lax.axis_index("rows"), 2)
    px = lax.rem(lax.axis_index("cols"), 2)
    pz = lax.rem(lax.axis_index("slabs"), 2)
    order = [mirrored(j, py, rows) for j in range(rows)]
    z_copies, copies = [], []
    for which in range(n_z):
        z = pl.multiple_of(near(which, pz, nz // SUB) * SUB, SUB)
        for j in range(rows):
            z_copies.append((tracer.at[order[j], :, pl.ds(z, SUB), :], groups.at[which, j]))
    for which in range(n_x):
        for j in range(rows):
            copies.append((tracer.at[order[j], near(which, px, nx)], x_faces[which].at[j]))
    for which in range(n_y):
        copies.append((tracer.at[order[rows - 1 if which == 0 else 0]], y_faces[which]))
    started = []
    for k, (src, dst) in enumerate(z_copies + copies):
        copy = pltpu.make_async_copy(src, dst, sems.at[k])
        copy.start()
        started.append(copy)
    for copy in started[: len(z_copies)]:
        copy.wait()
    for which in range(n_z):
        z = near(which, pz, SUB)
        for j in range(rows):
            cells = groups.at[which, j].reshape(nx * SUB, 128)
            for x in range(0, nx, SUB):
                face = cells[pl.ds(x * SUB + z, SUB, stride=SUB), :]
                z_faces[which][j, pl.ds(x, SUB), :] = face
    for copy in started[len(z_copies) :]:
        copy.wait()


def bulk_kernel(dims, counts, step, *refs):
    rows, nx, nz = dims
    first, last = step == 0, step == STEPS - 1
    src, refs = (refs[:1], refs[1:]) if first else (refs[:rows], refs[rows:])
    halos, refs = refs[: counts[0]], refs[counts[0] :]
    crowding, refs = refs[0], refs[1:]
    py = lax.rem(lax.axis_index("rows"), 2)
    order = [mirrored(j, py, rows) for j in range(rows)]
    pitch = nz + 1
    groups = nz // SUB
    together = 2 if groups % 4 == 0 else 1
    span = together * together * SUB
    piece = together * SUB
    blocks = nz // span
    copies = []
    if first:
        outs, (cells, sems) = refs[:rows], refs[rows:]
        for k in range(nz // piece):
            at = (slice(None), slice(None), pl.ds(k * piece, piece), slice(None))
            copies.append(pltpu.make_async_copy(src[0].at[at], cells.at[at], sems.at[k]))
            copies[-1].start()
    elif last:
        done, outs, sems = refs[0], refs[1 : 1 + rows], refs[1 + rows]
    else:
        outs = refs

    if not last:
        zero = jnp.zeros((SUB, 128), jnp.float32)
        for out in outs:
            for x in range(0, nx, SUB):
                out[pl.ds(x * pitch, SUB, stride=pitch), :] = zero
            out[pl.ds(nx * pitch, SUB), :] = zero

    scale = 2.0 * 10.0**-step

    def columns(z, edges):
        shifts = [z + k * together * SUB for k in range(together)]

        def load(k, j, x, shift):
            z = shifts[k]
            if first:
                ref = cells.at[order[j]]
                if shift == 0:
                    return ref[x, pl.ds(z, SUB), :]
                if edges[k] == shift:
                    own = ref[x, pl.ds(z, SUB), :]
                    rolled = pltpu.roll(own, (-shift) % SUB, 0)
                    row = lax.broadcasted_iota(jnp.int32, (SUB, 128), 0)
                    return jnp.where(row == (0 if shift < 0 else SUB - 1), 0.0, rolled)
                return ref[x, pl.ds(z + shift, SUB), :]
            return src[j][pl.ds(x * pitch + 1 + z + shift, SUB), :]

        def load_halo(k, which, x):
            if first:
                return halos[which][x, pl.ds(shifts[k], SUB), :]
            return halos[which][pl.ds(x * pitch + 1 + shifts[k], SUB), :]

        def plane(x):
            planes = [[load(k, j, x, 0) for j in range(rows)] for k in range(together)]
            above = [load_halo(k, 0, x) for k in range(together)]
            below = [load_halo(k, 1, x) if counts[0] > 1 else None for k in range(together)]
            return planes, above, below

        def advance(x, carry, final):
            diag, here, below = carry
            after = None if final else plane(x + 1)
            diags = []
            for k in range(together):
                forward = []
                for j in range(-1, rows):
                    own = below[k] if j < 0 else here[k][j]
                    if final:
                        forward.append(own)
                        continue
                    ahead = after[0][k][j + 1] if j + 1 < rows else after[1][k]
                    forward.append(ahead if own is None else own + ahead)
                for j in range(rows):
                    total = load(k, j, x, -1) + load(k, j, x, 1)
                    total = total + diag[k][j]
                    if forward[j] is not None:
                        total = total + forward[j]
                    cell = here[k][j]
                    c = crowding[order[j], x, pl.ds(shifts[k], SUB), :]
                    value = total + cell * (6.0 - (c * scale) * cell)
                    if last:
                        outs[j][x, pl.ds(shifts[k], SUB), :] = value * 10.0**-STEPS
                    else:
                        outs[j][pl.ds(x * pitch + 1 + shifts[k], SUB), :] = value
                diags.append(forward[1:])
            return None if final else (diags, after[0], after[2])

        planes, above, below = plane(0)
        carry = ([planes[k][1:] + [above[k]] for k in range(together)], planes, below)
        unroll = max(k for k in range(1, 10) if (nx - 1) % k == 0)

        def body(i, carry):
            for k in range(unroll):
                carry = advance(i * unroll + k, carry, False)
            return carry

        carry = lax.fori_loop(0, (nx - 1) // unroll, body, carry)
        advance(nx - 1, carry, True)

    def block(base, part, edges):
        columns(base + part * SUB, edges)

    parts = [(k, part) for k in range(blocks) for part in range(together)]
    if first:
        landed = 0
        for k, part in parts:
            base = k * span + part * SUB
            top = base + (together - 1) * piece + SUB
            edges = [0] * together
            if base == 0:
                edges[0] = -1
            if top == nz:
                edges[-1] = 1
            while landed * piece < min(top + 1, nz):
                copies[landed].wait()
                landed += 1
            block(k * span, part, edges)
    elif last:

        def send(group, j):
            at = (slice(None), pl.ds(pl.multiple_of(group * SUB, SUB), SUB), slice(None))
            return pltpu.make_async_copy(outs[j].at[at], done.at[order[j]].at[at], sems.at[group, j])

        @pl.loop(0, blocks)
        def _(k):
            for part in range(together):
                block(pl.multiple_of(k * span, SUB), part, None)
                for g in range(together):
                    for j in range(rows):
                        send(k * together * together + part + g * together, j).start()

        for group in range(groups):
            for j in range(rows):
                send(group, j).wait()
    else:

        @pl.loop(0, blocks)
        def _(k):
            for part in range(together):
                block(pl.multiple_of(k * span, SUB), part, None)


def patch_kernel(dims, counts, step, *refs):
    rows, nx, nz = dims
    last = step == STEPS - 1
    n_state = rows + 1 if last else rows
    n_x, n_z = counts[1], counts[2]
    refs = refs[n_state:]
    halo_x, halo_z, refs = refs[:n_x], refs[n_x : n_x + n_z], refs[n_x + n_z :]
    state, refs = refs[:n_state], refs[n_state:]
    if last:
        done, cells, sems = state[0], state[1:], refs[0]
    else:
        face_x, face_z = refs[:n_x], refs[n_x:]
    py = lax.rem(lax.axis_index("rows"), 2)
    px = lax.rem(lax.axis_index("cols"), 2)
    pz = lax.rem(lax.axis_index("slabs"), 2)
    pitch = nz if last else nz + 1
    offset = 0 if last else 1

    if last:
        order = [mirrored(j, py, rows) for j in range(rows)]
        views = [cells[j].reshape(nx * nz, 128) for j in range(rows)]
    else:
        views = state

    def scaled(values):
        return values * 10.0**-STEPS if last else values

    copies = []

    def send(j, at):
        sem = sems.at[len(copies)]
        copies.append(pltpu.make_async_copy(cells[j].at[at], done.at[order[j]].at[at], sem))
        copies[-1].start()

    for which in range(n_z):
        z = near(which, pz, nz)
        for j in range(rows):
            for x in range(0, nx, SUB):
                at = (pl.ds(x * pitch + offset + z, SUB, stride=pitch), slice(None))
                views[j][at] = views[j][at] + scaled(halo_z[which][j, pl.ds(x, SUB), :])
    for which in range(n_x):
        x = near(which, px, nx)
        for j in range(rows):
            for z in range(0, nz, SUB):
                at = (pl.ds(x * pitch + offset + z, SUB), slice(None))
                value = views[j][at] + scaled(halo_x[which][j, pl.ds(z, SUB), :])
                views[j][at] = value
                if not last:
                    face_x[which][j, pl.ds(z, SUB), :] = value
    if last:
        inner = pl.ds(SUB, nz - 2 * SUB)
        for j in range(rows):
            for z in (0, nz - SUB):
                send(j, (slice(None), pl.ds(z, SUB), slice(None)))
            for x in (0, nx - 1):
                send(j, (x, inner, slice(None)))
        for copy in copies:
            copy.wait()
        return
    for which in range(n_z):
        z = near(which, pz, nz)
        for j in range(rows):
            for x in range(0, nx, SUB):
                at = (pl.ds(x * pitch + offset + z, SUB, stride=pitch), slice(None))
                face_z[which][j, pl.ds(x, SUB), :] = views[j][at]


def call(kernel, name, out_shape, args, out_specs=None, in_specs=None, aliases=None, scratch=(), vmem=1):
    return pl.pallas_call(
        kernel,
        name=name,
        out_shape=out_shape,
        in_specs=in_specs or [VMEM_SPEC] * len(args),
        out_specs=out_specs or [VMEM_SPEC] * len(out_shape),
        input_output_aliases=aliases or {},
        scratch_shapes=list(scratch),
        compiler_params=pltpu.CompilerParams(vmem_limit_bytes=vmem * 1024 * 1024),
    )(*args)


def on_device(tracer, crowding):
    rows, nx, nz, species = tracer.shape
    dims = (rows, nx, nz)
    sizes = [lax.axis_size(axis) for axis in ("rows", "cols", "slabs")]
    counts = [len(matchings(size)) for size in sizes]
    pitch_rows = -(-(nx * (nz + 1) + SUB) // 32) * 32
    f32 = jnp.float32
    full_row = pltpu.VMEM((nx, nz, species), f32)
    state_row = pltpu.VMEM((pitch_rows, species), f32)
    x_face = pltpu.VMEM((rows, nz, species), f32)
    z_face = pltpu.VMEM((rows, nx, species), f32)

    out_shape = [full_row] * counts[0] + [x_face] * counts[1] + [z_face] * counts[2]
    packed = call(
        functools.partial(pack_kernel, dims, counts),
        "pack",
        out_shape,
        (pltpu.with_memory_space_constraint(tracer, pltpu.HBM),),
        in_specs=[HBM_SPEC],
        scratch=[
            pltpu.VMEM((counts[2], rows, nx, SUB, species), f32),
            pltpu.SemaphoreType.DMA((counts[0] + rows * (counts[1] + counts[2]),)),
        ],
        vmem=4,
    )
    y_faces, packed = packed[: counts[0]], packed[counts[0] :]
    x_faces, z_faces = packed[: counts[1]], packed[counts[1] :]
    state = [tracer]
    for step in range(STEPS):
        last = step == STEPS - 1
        y_halos = [swap(face, "rows", k, sizes[0]) for k, face in enumerate(y_faces)]
        x_halos = [swap(face, "cols", k, sizes[1]) for k, face in enumerate(x_faces)]
        z_halos = [swap(face, "slabs", k, sizes[2]) for k, face in enumerate(z_faces)]
        stage_sems = pltpu.SemaphoreType.DMA((nz // SUB,))
        kernel = functools.partial(bulk_kernel, dims, counts, step)
        args = (*state, *y_halos, crowding)
        if step == 0:
            args = (pltpu.with_memory_space_constraint(tracer, pltpu.HBM), *args[1:])
            state = call(
                kernel,
                "bulk0",
                [state_row] * rows,
                args,
                in_specs=[HBM_SPEC] + [VMEM_SPEC] * (len(args) - 1),
                scratch=[pltpu.VMEM(tracer.shape, f32), stage_sems],
                vmem=tracer.size * 4 // 2**20 + 1,
            )
        elif last:
            state = call(
                kernel,
                "bulk_last",
                [pltpu.HBM(tracer.shape, f32)] + [full_row] * rows,
                args,
                out_specs=[HBM_SPEC] + [VMEM_SPEC] * rows,
                scratch=[pltpu.SemaphoreType.DMA((nz // SUB, rows))],
            )
        else:
            state = call(kernel, f"bulk{step}", [state_row] * rows, args)
        kernel = functools.partial(patch_kernel, dims, counts, step)
        args = (*state, *x_halos, *z_halos)
        aliases = {k: k for k in range(len(state))}
        if last:
            specs = [HBM_SPEC] + [VMEM_SPEC] * rows
            return call(
                kernel,
                "patch_last",
                [pltpu.HBM(tracer.shape, f32)] + [full_row] * rows,
                args,
                in_specs=specs + [VMEM_SPEC] * (len(args) - len(specs)),
                out_specs=specs,
                aliases=aliases,
                scratch=[pltpu.SemaphoreType.DMA((4 * rows,))],
            )[0]
        out_shape = [state_row] * rows + [x_face] * counts[1] + [z_face] * counts[2]
        patched = call(kernel, f"patch{step}", out_shape, args, aliases=aliases)
        state = patched[:rows]
        y_faces = [state[rows - 1 if k == 0 else 0] for k in range(counts[0])]
        x_faces = patched[rows : rows + counts[1]]
        z_faces = patched[rows + counts[1] :]


def solution(mesh):
    placed = (P("rows", "cols", "slabs", None), P("rows", "cols", "slabs", None))
    return jax.shard_map(
        on_device,
        mesh=mesh,
        in_specs=placed,
        out_specs=P("rows", "cols", "slabs", None),
        check_vma=False,
    )
```

```python
import functools

import jax
import jax.numpy as jnp
from jax import lax
from jax.experimental import pallas as pl
from jax.experimental.pallas import tpu as pltpu
from jax.sharding import PartitionSpec as P

STEPS = 4
SUB = 8
VMEM_SPEC = pl.BlockSpec(memory_space=pltpu.VMEM)
HBM_SPEC = pl.BlockSpec(memory_space=pltpu.HBM)


def matchings(count):
    swaps = []
    for first in (0, 1):
        pairs = [(i, i + 1) for i in range(first, count - 1, 2)]
        if pairs:
            swaps.append(pairs + [(b, a) for a, b in pairs])
    return swaps


def swap(face, axis, which, count):
    with jax.named_scope(f"swap_{axis}_{which}"):
        return lax.ppermute(face, axis, matchings(count)[which])


def near(which, parity, size):
    high = parity == which
    return jnp.where(high, size - 1, 0)


def mirrored(j, parity, rows):
    return jnp.where(parity == 0, j, rows - 1 - j)


def face_rows(n_y, rows):
    return {rows - 1 if which == 0 else 0: which for which in range(n_y)}


def pack_kernel(dims, counts, tracer, *refs):
    rows, nx, nz = dims
    n_y, n_x, n_z = counts
    faces, (groups, sems) = refs[: sum(counts)], refs[sum(counts) :]
    y_faces, x_faces, z_faces = faces[:n_y], faces[n_y : n_y + n_x], faces[n_y + n_x :]
    py = lax.rem(lax.axis_index("rows"), 2)
    px = lax.rem(lax.axis_index("cols"), 2)
    pz = lax.rem(lax.axis_index("slabs"), 2)
    order = [mirrored(j, py, rows) for j in range(rows)]
    z_copies, copies = [], []
    for which in range(n_z):
        z = pl.multiple_of(near(which, pz, nz // SUB) * SUB, SUB)
        for j in range(rows):
            z_copies.append((tracer.at[order[j], :, pl.ds(z, SUB), :], groups.at[which, j]))
    for which in range(n_x):
        for j in range(rows):
            copies.append((tracer.at[order[j], near(which, px, nx)], x_faces[which].at[j]))
    for which in range(n_y):
        copies.append((tracer.at[order[rows - 1 if which == 0 else 0]], y_faces[which]))
    started = []
    for k, (src, dst) in enumerate(z_copies + copies):
        copy = pltpu.make_async_copy(src, dst, sems.at[k])
        copy.start()
        started.append(copy)
    for copy in started[: len(z_copies)]:
        copy.wait()
    for which in range(n_z):
        z = near(which, pz, SUB)
        for j in range(rows):
            cells = groups.at[which, j].reshape(nx * SUB, 128)
            for x in range(0, nx, SUB):
                face = cells[pl.ds(x * SUB + z, SUB, stride=SUB), :]
                z_faces[which][j, pl.ds(x, SUB), :] = face
    for copy in started[len(z_copies) :]:
        copy.wait()


def together_of(nz):
    return 2 if nz // SUB % 4 == 0 else 1


def late_groups(nz):
    groups, together = nz // SUB, together_of(nz)
    return {0, *range(groups - 1 - together * (together - 1), groups, together)}


def bulk_kernel(dims, counts, step, *refs):
    rows, nx, nz = dims
    first, last = step == 0, step == STEPS - 1
    n_src = 1 + counts[0] if first else rows
    src, refs = refs[:n_src], refs[n_src:]
    halos, refs = refs[: counts[0]], refs[counts[0] :]
    crowding, refs = refs[0], refs[1:]
    py = lax.rem(lax.axis_index("rows"), 2)
    order = [mirrored(j, py, rows) for j in range(rows)]
    pitch = nz + 1
    groups = nz // SUB
    together = together_of(nz)
    span = together * together * SUB
    piece = together * SUB
    blocks = nz // span
    copies = []
    if first:
        outs, (cells, sems) = refs[:rows], refs[rows:]
        held = face_rows(counts[0], rows)
        fetched = [j for j in range(rows) if j not in held]
        planes_of = [src[1 + held[j]] if j in held else cells.at[fetched.index(j)] for j in range(rows)]
        for k in range(nz // piece):
            for n, j in enumerate(fetched):
                at = (slice(None), pl.ds(k * piece, piece), slice(None))
                dst = cells.at[n].at[at]
                copies.append(pltpu.make_async_copy(src[0].at[order[j]].at[at], dst, sems.at[k, n]))
                copies[-1].start()
    elif last:
        done, outs, sems = refs[0], refs[1 : 1 + rows], refs[1 + rows]
    else:
        outs = refs

    if not last:
        zero = jnp.zeros((SUB, 128), jnp.float32)
        for out in outs:
            for x in range(0, nx, SUB):
                out[pl.ds(x * pitch, SUB, stride=pitch), :] = zero
            out[pl.ds(nx * pitch, SUB), :] = zero

    scale = 2.0 * 10.0**-step

    def columns(z, edges):
        shifts = [z + k * together * SUB for k in range(together)]

        def load(k, j, x, shift):
            z = shifts[k]
            if first:
                ref = planes_of[j]
                if shift == 0:
                    return ref[x, pl.ds(z, SUB), :]
                if edges[k] == shift:
                    own = ref[x, pl.ds(z, SUB), :]
                    rolled = pltpu.roll(own, (-shift) % SUB, 0)
                    row = lax.broadcasted_iota(jnp.int32, (SUB, 128), 0)
                    return jnp.where(row == (0 if shift < 0 else SUB - 1), 0.0, rolled)
                return ref[x, pl.ds(z + shift, SUB), :]
            return src[j][pl.ds(x * pitch + 1 + z + shift, SUB), :]

        def load_halo(k, which, x):
            if first:
                return halos[which][x, pl.ds(shifts[k], SUB), :]
            return halos[which][pl.ds(x * pitch + 1 + shifts[k], SUB), :]

        def plane(x):
            planes = [[load(k, j, x, 0) for j in range(rows)] for k in range(together)]
            above = [load_halo(k, 0, x) for k in range(together)]
            below = [load_halo(k, 1, x) if counts[0] > 1 else None for k in range(together)]
            return planes, above, below

        def advance(x, carry, final):
            diag, here, below = carry
            after = None if final else plane(x + 1)
            diags = []
            for k in range(together):
                forward = []
                for j in range(-1, rows):
                    own = below[k] if j < 0 else here[k][j]
                    if final:
                        forward.append(own)
                        continue
                    ahead = after[0][k][j + 1] if j + 1 < rows else after[1][k]
                    forward.append(ahead if own is None else own + ahead)
                for j in range(rows):
                    total = load(k, j, x, -1) + load(k, j, x, 1)
                    total = total + diag[k][j]
                    if forward[j] is not None:
                        total = total + forward[j]
                    cell = here[k][j]
                    c = crowding[order[j], x, pl.ds(shifts[k], SUB), :]
                    value = total + cell * (6.0 - (c * scale) * cell)
                    if last:
                        outs[j][x, pl.ds(shifts[k], SUB), :] = value * 10.0**-STEPS
                    else:
                        outs[j][pl.ds(x * pitch + 1 + shifts[k], SUB), :] = value
                diags.append(forward[1:])
            return None if final else (diags, after[0], after[2])

        planes, above, below = plane(0)
        carry = ([planes[k][1:] + [above[k]] for k in range(together)], planes, below)
        unroll = max(k for k in range(1, 10) if (nx - 1) % k == 0)

        def body(i, carry):
            for k in range(unroll):
                carry = advance(i * unroll + k, carry, False)
            return carry

        carry = lax.fori_loop(0, (nx - 1) // unroll, body, carry)
        advance(nx - 1, carry, True)

    def block(base, part, edges):
        columns(base + part * SUB, edges)

    parts = [(k, part) for k in range(blocks) for part in range(together)]
    if first:
        landed = 0
        for k, part in parts:
            base = k * span + part * SUB
            top = base + (together - 1) * piece + SUB
            edges = [0] * together
            if base == 0:
                edges[0] = -1
            if top == nz:
                edges[-1] = 1
            while landed * piece < min(top + 1, nz):
                for n in range(len(fetched)):
                    copies[landed * len(fetched) + n].wait()
                landed += 1
            block(k * span, part, edges)
    elif last:

        def send(group, j):
            at = (slice(None), pl.ds(pl.multiple_of(group * SUB, SUB), SUB), slice(None))
            return pltpu.make_async_copy(outs[j].at[at], done.at[order[j]].at[at], sems.at[group, j])

        @pl.loop(0, blocks)
        def _(k):
            for part in range(together):
                block(pl.multiple_of(k * span, SUB), part, None)
                for g in range(together):
                    group = k * together * together + part + g * together
                    early = [group != left for left in late_groups(nz)]

                    @pl.when(functools.reduce(jnp.logical_and, early))
                    def _():
                        for j in range(rows):
                            send(group, j).start()

        for group in range(groups):
            if group not in late_groups(nz):
                for j in range(rows):
                    send(group, j).wait()
    else:

        @pl.loop(0, blocks)
        def _(k):
            for part in range(together):
                block(pl.multiple_of(k * span, SUB), part, None)


def patch_kernel(dims, counts, step, *refs):
    rows, nx, nz = dims
    last = step == STEPS - 1
    n_state = rows + 1 if last else rows
    n_x, n_z = counts[1], counts[2]
    refs = refs[n_state:]
    halo_x, halo_z, refs = refs[:n_x], refs[n_x : n_x + n_z], refs[n_x + n_z :]
    state, refs = refs[:n_state], refs[n_state:]
    if last:
        done, cells, sems = state[0], state[1:], refs[0]
    else:
        face_x, face_z = refs[:n_x], refs[n_x:]
    py = lax.rem(lax.axis_index("rows"), 2)
    px = lax.rem(lax.axis_index("cols"), 2)
    pz = lax.rem(lax.axis_index("slabs"), 2)
    pitch = nz if last else nz + 1
    offset = 0 if last else 1

    if last:
        order = [mirrored(j, py, rows) for j in range(rows)]
        views = [cells[j].reshape(nx * nz, 128) for j in range(rows)]
    else:
        views = state

    def scaled(values):
        return values * 10.0**-STEPS if last else values

    copies = []

    def send(j, at):
        sem = sems.at[len(copies)]
        copies.append(pltpu.make_async_copy(cells[j].at[at], done.at[order[j]].at[at], sem))
        copies[-1].start()

    def patch_z(which):
        z = near(which, pz, nz)
        for j in range(rows):
            for x in range(0, nx, SUB):
                at = (pl.ds(x * pitch + offset + z, SUB, stride=pitch), slice(None))
                views[j][at] = views[j][at] + scaled(halo_z[which][j, pl.ds(x, SUB), :])

    def patch_x(which):
        x = near(which, px, nx)
        for j in range(rows):
            for z in range(0, nz, SUB):
                at = (pl.ds(x * pitch + offset + z, SUB), slice(None))
                value = views[j][at] + scaled(halo_x[which][j, pl.ds(z, SUB), :])
                views[j][at] = value
                if not last:
                    face_x[which][j, pl.ds(z, SUB), :] = value

    if last:
        for group in sorted(late_groups(nz) - {0, nz // SUB - 1}):
            for j in range(rows):
                send(j, (pl.ds(1, nx - 2), pl.ds(group * SUB, SUB), slice(None)))
        for which in range(2):
            if which < n_x:
                patch_x(which)
            for j in range(rows):
                send(j, (near(which, px, nx), pl.ds(SUB, nz - 2 * SUB), slice(None)))
        for which in range(2):
            if which < n_z:
                patch_z(which)
            z = pl.multiple_of(near(which, pz, nz // SUB) * SUB, SUB)
            for j in range(rows):
                send(j, (slice(None), pl.ds(z, SUB), slice(None)))
        for copy in copies:
            copy.wait()
        return
    for which in range(n_z):
        patch_z(which)
    for which in range(n_x):
        patch_x(which)
    for which in range(n_z):
        z = near(which, pz, nz)
        for j in range(rows):
            for x in range(0, nx, SUB):
                at = (pl.ds(x * pitch + offset + z, SUB, stride=pitch), slice(None))
                face_z[which][j, pl.ds(x, SUB), :] = views[j][at]


def call(kernel, name, out_shape, args, out_specs=None, in_specs=None, aliases=None, scratch=(), vmem=1):
    return pl.pallas_call(
        kernel,
        name=name,
        out_shape=out_shape,
        in_specs=in_specs or [VMEM_SPEC] * len(args),
        out_specs=out_specs or [VMEM_SPEC] * len(out_shape),
        input_output_aliases=aliases or {},
        scratch_shapes=list(scratch),
        compiler_params=pltpu.CompilerParams(vmem_limit_bytes=vmem * 1024 * 1024),
    )(*args)


def on_device(tracer, crowding):
    rows, nx, nz, species = tracer.shape
    dims = (rows, nx, nz)
    sizes = [lax.axis_size(axis) for axis in ("rows", "cols", "slabs")]
    counts = [len(matchings(size)) for size in sizes]
    pitch_rows = -(-(nx * (nz + 1) + SUB) // 32) * 32
    f32 = jnp.float32
    full_row = pltpu.VMEM((nx, nz, species), f32)
    state_row = pltpu.VMEM((pitch_rows, species), f32)
    x_face = pltpu.VMEM((rows, nz, species), f32)
    z_face = pltpu.VMEM((rows, nx, species), f32)

    out_shape = [full_row] * counts[0] + [x_face] * counts[1] + [z_face] * counts[2]
    packed = call(
        functools.partial(pack_kernel, dims, counts),
        "pack",
        out_shape,
        (pltpu.with_memory_space_constraint(tracer, pltpu.HBM),),
        in_specs=[HBM_SPEC],
        scratch=[
            pltpu.VMEM((counts[2], rows, nx, SUB, species), f32),
            pltpu.SemaphoreType.DMA((counts[0] + rows * (counts[1] + counts[2]),)),
        ],
        vmem=4,
    )
    y_faces, packed = packed[: counts[0]], packed[counts[0] :]
    x_faces, z_faces = packed[: counts[1]], packed[counts[1] :]
    state = [tracer]
    for step in range(STEPS):
        last = step == STEPS - 1
        y_halos = [swap(face, "rows", k, sizes[0]) for k, face in enumerate(y_faces)]
        x_halos = [swap(face, "cols", k, sizes[1]) for k, face in enumerate(x_faces)]
        z_halos = [swap(face, "slabs", k, sizes[2]) for k, face in enumerate(z_faces)]
        kernel = functools.partial(bulk_kernel, dims, counts, step)
        args = (*state, *y_halos, crowding)
        if step == 0:
            args = (pltpu.with_memory_space_constraint(tracer, pltpu.HBM), *y_faces, *args[1:])
            fetched = rows - len(face_rows(counts[0], rows))
            state = call(
                kernel,
                "bulk0",
                [state_row] * rows,
                args,
                in_specs=[HBM_SPEC] + [VMEM_SPEC] * (len(args) - 1),
                scratch=[
                    pltpu.VMEM((fetched, nx, nz, species), f32),
                    pltpu.SemaphoreType.DMA((nz // SUB, fetched)),
                ],
                vmem=tracer.size // rows * fetched * 4 // 2**20 + 1,
            )
        elif last:
            state = call(
                kernel,
                "bulk_last",
                [pltpu.HBM(tracer.shape, f32)] + [full_row] * rows,
                args,
                out_specs=[HBM_SPEC] + [VMEM_SPEC] * rows,
                scratch=[pltpu.SemaphoreType.DMA((nz // SUB, rows))],
            )
        else:
            state = call(kernel, f"bulk{step}", [state_row] * rows, args)
        kernel = functools.partial(patch_kernel, dims, counts, step)
        args = (*state, *x_halos, *z_halos)
        aliases = {k: k for k in range(len(state))}
        if last:
            specs = [HBM_SPEC] + [VMEM_SPEC] * rows
            return call(
                kernel,
                "patch_last",
                [pltpu.HBM(tracer.shape, f32)] + [full_row] * rows,
                args,
                in_specs=specs + [VMEM_SPEC] * (len(args) - len(specs)),
                out_specs=specs,
                aliases=aliases,
                scratch=[pltpu.SemaphoreType.DMA(((2 + len(late_groups(nz))) * rows,))],
            )[0]
        out_shape = [state_row] * rows + [x_face] * counts[1] + [z_face] * counts[2]
        patched = call(kernel, f"patch{step}", out_shape, args, aliases=aliases)
        state = patched[:rows]
        y_faces = [state[rows - 1 if k == 0 else 0] for k in range(counts[0])]
        x_faces = patched[rows : rows + counts[1]]
        z_faces = patched[rows + counts[1] :]


def solution(mesh):
    placed = (P("rows", "cols", "slabs", None), P("rows", "cols", "slabs", None))
    return jax.shard_map(
        on_device,
        mesh=mesh,
        in_specs=placed,
        out_specs=P("rows", "cols", "slabs", None),
        check_vma=False,
    )
```

```python
import functools

import jax
import jax.numpy as jnp
from jax import lax
from jax.experimental import pallas as pl
from jax.experimental.pallas import tpu as pltpu
from jax.sharding import PartitionSpec as P

STEPS = 4
SUB = 8
VMEM_SPEC = pl.BlockSpec(memory_space=pltpu.VMEM)
HBM_SPEC = pl.BlockSpec(memory_space=pltpu.HBM)


def matchings(count):
    swaps = []
    for first in (0, 1):
        pairs = [(i, i + 1) for i in range(first, count - 1, 2)]
        if pairs:
            swaps.append(pairs + [(b, a) for a, b in pairs])
    return swaps


def swap(face, axis, which, count):
    with jax.named_scope(f"swap_{axis}_{which}"):
        return lax.ppermute(face, axis, matchings(count)[which])


def near(which, parity, size):
    high = parity == which
    return jnp.where(high, size - 1, 0)


def mirrored(j, parity, rows):
    return jnp.where(parity == 0, j, rows - 1 - j)


def face_rows(n_y, rows):
    return {rows - 1 if which == 0 else 0: which for which in range(n_y)}


def pack_kernel(dims, counts, tracer, *refs):
    rows, nx, nz = dims
    n_y, n_x, n_z = counts
    faces, sems = refs[: sum(counts)], refs[sum(counts)]
    y_faces, x_faces, z_faces = faces[:n_y], faces[n_y : n_y + n_x], faces[n_y + n_x :]
    py = lax.rem(lax.axis_index("rows"), 2)
    px = lax.rem(lax.axis_index("cols"), 2)
    pz = lax.rem(lax.axis_index("slabs"), 2)
    order = [mirrored(j, py, rows) for j in range(rows)]
    copies = []
    for which in range(n_x):
        for j in range(rows):
            copies.append((tracer.at[order[j], near(which, px, nx)], x_faces[which].at[j]))
    for which in range(n_z):
        for j in range(rows):
            copies.append((tracer.at[order[j], :, near(which, pz, nz)], z_faces[which].at[j]))
    for which in range(n_y):
        copies.append((tracer.at[order[rows - 1 if which == 0 else 0]], y_faces[which]))
    started = []
    for k, (src, dst) in enumerate(copies):
        copy = pltpu.make_async_copy(src, dst, sems.at[k])
        copy.start()
        started.append(copy)
    for copy in started:
        copy.wait()


def together_of(nz):
    return 2 if nz // SUB % 4 == 0 else 1


def late_groups(nz):
    groups, together = nz // SUB, together_of(nz)
    return {0, *range(groups - 1 - together * (together - 1), groups, together)}


def bulk_kernel(dims, counts, step, *refs):
    rows, nx, nz = dims
    first, last = step == 0, step == STEPS - 1
    n_src = 1 + counts[0] if first else rows
    src, refs = refs[:n_src], refs[n_src:]
    halos, refs = refs[: counts[0]], refs[counts[0] :]
    crowding, refs = refs[0], refs[1:]
    py = lax.rem(lax.axis_index("rows"), 2)
    order = [mirrored(j, py, rows) for j in range(rows)]
    pitch = nz + 1
    groups = nz // SUB
    together = together_of(nz)
    span = together * together * SUB
    piece = together * SUB
    blocks = nz // span
    copies = []
    if first:
        outs, (cells, sems) = refs[:rows], refs[rows:]
        held = face_rows(counts[0], rows)
        fetched = [j for j in range(rows) if j not in held]
        planes_of = [src[1 + held[j]] if j in held else cells.at[fetched.index(j)] for j in range(rows)]
        for k in range(nz // piece):
            for n, j in enumerate(fetched):
                at = (slice(None), pl.ds(k * piece, piece), slice(None))
                dst = cells.at[n].at[at]
                copies.append(pltpu.make_async_copy(src[0].at[order[j]].at[at], dst, sems.at[k, n]))
                copies[-1].start()
    elif last:
        done, outs, sems = refs[0], refs[1 : 1 + rows], refs[1 + rows]
    else:
        outs = refs

    if not last:
        zero = jnp.zeros((SUB, 128), jnp.float32)
        for out in outs:
            for x in range(0, nx, SUB):
                out[pl.ds(x * pitch, SUB, stride=pitch), :] = zero
            out[pl.ds(nx * pitch, SUB), :] = zero

    scale = 2.0 * 10.0**-step

    def columns(z, edges):
        shifts = [z + k * together * SUB for k in range(together)]

        def load(k, j, x, shift):
            z = shifts[k]
            if first:
                ref = planes_of[j]
                if shift == 0:
                    return ref[x, pl.ds(z, SUB), :]
                if edges[k] == shift:
                    own = ref[x, pl.ds(z, SUB), :]
                    rolled = pltpu.roll(own, (-shift) % SUB, 0)
                    row = lax.broadcasted_iota(jnp.int32, (SUB, 128), 0)
                    return jnp.where(row == (0 if shift < 0 else SUB - 1), 0.0, rolled)
                return ref[x, pl.ds(z + shift, SUB), :]
            return src[j][pl.ds(x * pitch + 1 + z + shift, SUB), :]

        def load_halo(k, which, x):
            if first:
                return halos[which][x, pl.ds(shifts[k], SUB), :]
            return halos[which][pl.ds(x * pitch + 1 + shifts[k], SUB), :]

        def plane(x):
            planes = [[load(k, j, x, 0) for j in range(rows)] for k in range(together)]
            above = [load_halo(k, 0, x) for k in range(together)]
            below = [load_halo(k, 1, x) if counts[0] > 1 else None for k in range(together)]
            return planes, above, below

        def advance(x, carry, final):
            diag, here, below = carry
            after = None if final else plane(x + 1)
            diags = []
            for k in range(together):
                forward = []
                for j in range(-1, rows):
                    own = below[k] if j < 0 else here[k][j]
                    if final:
                        forward.append(own)
                        continue
                    ahead = after[0][k][j + 1] if j + 1 < rows else after[1][k]
                    forward.append(ahead if own is None else own + ahead)
                for j in range(rows):
                    total = load(k, j, x, -1) + load(k, j, x, 1)
                    total = total + diag[k][j]
                    if forward[j] is not None:
                        total = total + forward[j]
                    cell = here[k][j]
                    c = crowding[order[j], x, pl.ds(shifts[k], SUB), :]
                    value = total + cell * (6.0 - (c * scale) * cell)
                    if last:
                        outs[j][x, pl.ds(shifts[k], SUB), :] = value * 10.0**-STEPS
                    else:
                        outs[j][pl.ds(x * pitch + 1 + shifts[k], SUB), :] = value
                diags.append(forward[1:])
            return None if final else (diags, after[0], after[2])

        planes, above, below = plane(0)
        carry = ([planes[k][1:] + [above[k]] for k in range(together)], planes, below)
        unroll = max(k for k in range(1, 22) if (nx - 1) % k == 0)

        def body(i, carry):
            for k in range(unroll):
                carry = advance(i * unroll + k, carry, False)
            return carry

        carry = lax.fori_loop(0, (nx - 1) // unroll, body, carry)
        advance(nx - 1, carry, True)

    def block(base, part, edges):
        columns(base + part * SUB, edges)

    parts = [(k, part) for k in range(blocks) for part in range(together)]
    if first:
        landed = 0
        for k, part in parts:
            base = k * span + part * SUB
            top = base + (together - 1) * piece + SUB
            edges = [0] * together
            if base == 0:
                edges[0] = -1
            if top == nz:
                edges[-1] = 1
            while landed * piece < min(top + 1, nz):
                for n in range(len(fetched)):
                    copies[landed * len(fetched) + n].wait()
                landed += 1
            block(k * span, part, edges)
    elif last:

        def send(group, j):
            at = (slice(None), pl.ds(pl.multiple_of(group * SUB, SUB), SUB), slice(None))
            return pltpu.make_async_copy(outs[j].at[at], done.at[order[j]].at[at], sems.at[group, j])

        @pl.loop(0, blocks)
        def _(k):
            for part in range(together):
                block(pl.multiple_of(k * span, SUB), part, None)
                for g in range(together):
                    group = k * together * together + part + g * together
                    early = [group != left for left in late_groups(nz)]

                    @pl.when(functools.reduce(jnp.logical_and, early))
                    def _():
                        for j in range(rows):
                            send(group, j).start()

        for group in range(groups):
            if group not in late_groups(nz):
                for j in range(rows):
                    send(group, j).wait()
    else:

        @pl.loop(0, blocks)
        def _(k):
            for part in range(together):
                block(pl.multiple_of(k * span, SUB), part, None)


def patch_kernel(dims, counts, step, *refs):
    rows, nx, nz = dims
    last = step == STEPS - 1
    n_state = rows + 1 if last else rows
    n_x, n_z = counts[1], counts[2]
    refs = refs[n_state:]
    halo_x, halo_z, refs = refs[:n_x], refs[n_x : n_x + n_z], refs[n_x + n_z :]
    state, refs = refs[:n_state], refs[n_state:]
    if last:
        done, cells, sems = state[0], state[1:], refs[0]
    else:
        face_x, face_z = refs[:n_x], refs[n_x:]
    py = lax.rem(lax.axis_index("rows"), 2)
    px = lax.rem(lax.axis_index("cols"), 2)
    pz = lax.rem(lax.axis_index("slabs"), 2)
    pitch = nz if last else nz + 1
    offset = 0 if last else 1

    if last:
        order = [mirrored(j, py, rows) for j in range(rows)]
        views = [cells[j].reshape(nx * nz, 128) for j in range(rows)]
    else:
        views = state

    def scaled(values):
        return values * 10.0**-STEPS if last else values

    copies = []

    def send(j, at):
        sem = sems.at[len(copies)]
        copies.append(pltpu.make_async_copy(cells[j].at[at], done.at[order[j]].at[at], sem))
        copies[-1].start()

    def patch_z(which):
        z = near(which, pz, nz)
        for j in range(rows):
            for x in range(0, nx, SUB):
                at = (pl.ds(x * pitch + offset + z, SUB, stride=pitch), slice(None))
                views[j][at] = views[j][at] + scaled(halo_z[which][j, pl.ds(x, SUB), :])

    def patch_x(which):
        x = near(which, px, nx)
        for j in range(rows):
            for z in range(0, nz, SUB):
                at = (pl.ds(x * pitch + offset + z, SUB), slice(None))
                value = views[j][at] + scaled(halo_x[which][j, pl.ds(z, SUB), :])
                views[j][at] = value
                if not last:
                    face_x[which][j, pl.ds(z, SUB), :] = value

    if last:
        for group in sorted(late_groups(nz) - {0, nz // SUB - 1}):
            for j in range(rows):
                send(j, (pl.ds(1, nx - 2), pl.ds(group * SUB, SUB), slice(None)))
        for which in range(2):
            if which < n_x:
                patch_x(which)
            for j in range(rows):
                send(j, (near(which, px, nx), pl.ds(SUB, nz - 2 * SUB), slice(None)))
        for which in range(2):
            if which < n_z:
                patch_z(which)
            z = pl.multiple_of(near(which, pz, nz // SUB) * SUB, SUB)
            for j in range(rows):
                send(j, (slice(None), pl.ds(z, SUB), slice(None)))
        for copy in copies:
            copy.wait()
        return
    for which in range(n_z):
        patch_z(which)
    for which in range(n_x):
        patch_x(which)
    for which in range(n_z):
        z = near(which, pz, nz)
        for j in range(rows):
            for x in range(0, nx, SUB):
                at = (pl.ds(x * pitch + offset + z, SUB, stride=pitch), slice(None))
                face_z[which][j, pl.ds(x, SUB), :] = views[j][at]


def call(kernel, name, out_shape, args, out_specs=None, in_specs=None, aliases=None, scratch=(), vmem=1):
    return pl.pallas_call(
        kernel,
        name=name,
        out_shape=out_shape,
        in_specs=in_specs or [VMEM_SPEC] * len(args),
        out_specs=out_specs or [VMEM_SPEC] * len(out_shape),
        input_output_aliases=aliases or {},
        scratch_shapes=list(scratch),
        compiler_params=pltpu.CompilerParams(vmem_limit_bytes=vmem * 1024 * 1024),
    )(*args)


def on_device(tracer, crowding):
    rows, nx, nz, species = tracer.shape
    dims = (rows, nx, nz)
    sizes = [lax.axis_size(axis) for axis in ("rows", "cols", "slabs")]
    counts = [len(matchings(size)) for size in sizes]
    pitch_rows = -(-(nx * (nz + 1) + SUB) // 32) * 32
    f32 = jnp.float32
    full_row = pltpu.VMEM((nx, nz, species), f32)
    state_row = pltpu.VMEM((pitch_rows, species), f32)
    x_face = pltpu.VMEM((rows, nz, species), f32)
    z_face = pltpu.VMEM((rows, nx, species), f32)

    thin = [(nx, nz, 1, species)] * counts[0] + [(rows, nz, 1, species)] * counts[1]
    thin += [(rows, nx, 1, species)] * counts[2]
    packed = call(
        functools.partial(pack_kernel, dims, counts),
        "pack",
        [pltpu.VMEM(shape, f32) for shape in thin],
        (pltpu.with_memory_space_constraint(tracer.reshape(rows, nx, nz, 1, species), pltpu.HBM),),
        in_specs=[HBM_SPEC],
        scratch=[pltpu.SemaphoreType.DMA((counts[0] + rows * (counts[1] + counts[2]),))],
    )
    packed = [face.reshape(face.shape[0], face.shape[1], species) for face in packed]
    y_faces, packed = packed[: counts[0]], packed[counts[0] :]
    x_faces, z_faces = packed[: counts[1]], packed[counts[1] :]
    state = [tracer]
    for step in range(STEPS):
        last = step == STEPS - 1
        y_halos = [swap(face, "rows", k, sizes[0]) for k, face in enumerate(y_faces)]
        x_halos = [swap(face, "cols", k, sizes[1]) for k, face in enumerate(x_faces)]
        z_halos = [swap(face, "slabs", k, sizes[2]) for k, face in enumerate(z_faces)]
        kernel = functools.partial(bulk_kernel, dims, counts, step)
        args = (*state, *y_halos, crowding)
        if step == 0:
            args = (pltpu.with_memory_space_constraint(tracer, pltpu.HBM), *y_faces, *args[1:])
            fetched = rows - len(face_rows(counts[0], rows))
            state = call(
                kernel,
                "bulk0",
                [state_row] * rows,
                args,
                in_specs=[HBM_SPEC] + [VMEM_SPEC] * (len(args) - 1),
                scratch=[
                    pltpu.VMEM((fetched, nx, nz, species), f32),
                    pltpu.SemaphoreType.DMA((nz // SUB, fetched)),
                ],
                vmem=tracer.size // rows * fetched * 4 // 2**20 + 1,
            )
        elif last:
            state = call(
                kernel,
                "bulk_last",
                [pltpu.HBM(tracer.shape, f32)] + [full_row] * rows,
                args,
                out_specs=[HBM_SPEC] + [VMEM_SPEC] * rows,
                scratch=[pltpu.SemaphoreType.DMA((nz // SUB, rows))],
            )
        else:
            state = call(kernel, f"bulk{step}", [state_row] * rows, args)
        kernel = functools.partial(patch_kernel, dims, counts, step)
        args = (*state, *x_halos, *z_halos)
        aliases = {k: k for k in range(len(state))}
        if last:
            specs = [HBM_SPEC] + [VMEM_SPEC] * rows
            return call(
                kernel,
                "patch_last",
                [pltpu.HBM(tracer.shape, f32)] + [full_row] * rows,
                args,
                in_specs=specs + [VMEM_SPEC] * (len(args) - len(specs)),
                out_specs=specs,
                aliases=aliases,
                scratch=[pltpu.SemaphoreType.DMA(((2 + len(late_groups(nz))) * rows,))],
            )[0]
        out_shape = [state_row] * rows + [x_face] * counts[1] + [z_face] * counts[2]
        patched = call(kernel, f"patch{step}", out_shape, args, aliases=aliases)
        state = patched[:rows]
        y_faces = [state[rows - 1 if k == 0 else 0] for k in range(counts[0])]
        x_faces = patched[rows : rows + counts[1]]
        z_faces = patched[rows + counts[1] :]


def solution(mesh):
    placed = (P("rows", "cols", "slabs", None), P("rows", "cols", "slabs", None))
    return jax.shard_map(
        on_device,
        mesh=mesh,
        in_specs=placed,
        out_specs=P("rows", "cols", "slabs", None),
        check_vma=False,
    )
```

```python
import functools

import jax
import jax.numpy as jnp
from jax import lax
from jax.experimental import pallas as pl
from jax.experimental.pallas import tpu as pltpu
from jax.sharding import PartitionSpec as P

STEPS = 4
SUB = 8
VMEM_SPEC = pl.BlockSpec(memory_space=pltpu.VMEM)
HBM_SPEC = pl.BlockSpec(memory_space=pltpu.HBM)


def matchings(count):
    swaps = []
    for first in (0, 1):
        pairs = [(i, i + 1) for i in range(first, count - 1, 2)]
        if pairs:
            swaps.append(pairs + [(b, a) for a, b in pairs])
    return swaps


def swap(face, axis, which, count):
    with jax.named_scope(f"swap_{axis}_{which}"):
        return lax.ppermute(face, axis, matchings(count)[which])


def near(which, parity, size):
    high = parity == which
    return jnp.where(high, size - 1, 0)


def mirrored(j, parity, rows):
    return jnp.where(parity == 0, j, rows - 1 - j)


def face_rows(n_y, rows):
    return {rows - 1 if which == 0 else 0: which for which in range(n_y)}


def fetched_rows(n_y, rows):
    return [j for j in range(rows) if j not in face_rows(n_y, rows)]


def preloaded(nz):
    return min(together_of(nz) * 2 * SUB, nz)


def pack_kernel(dims, counts, tracer, *refs):
    rows, nx, nz = dims
    n_y, n_x, n_z = counts
    faces, (cells, sems) = refs[: sum(counts)], refs[sum(counts) :]
    y_faces, x_faces, z_faces = faces[:n_y], faces[n_y : n_y + n_x], faces[n_y + n_x :]
    py = lax.rem(lax.axis_index("rows"), 2)
    px = lax.rem(lax.axis_index("cols"), 2)
    pz = lax.rem(lax.axis_index("slabs"), 2)
    order = [mirrored(j, py, rows) for j in range(rows)]
    copies = []
    for which in range(n_x):
        for j in range(rows):
            copies.append((tracer.at[order[j], near(which, px, nx)], x_faces[which].at[j]))
    for which in range(n_z):
        for j in range(rows):
            copies.append((tracer.at[order[j], :, near(which, pz, nz)], z_faces[which].at[j]))
    for which in range(n_y):
        copies.append((tracer.at[order[rows - 1 if which == 0 else 0]], y_faces[which]))
    ahead = pl.ds(0, preloaded(nz))
    for n, j in enumerate(fetched_rows(n_y, rows)):
        copies.append((tracer.at[order[j], :, ahead], cells.at[n, :, ahead]))
    started = []
    for k, (src, dst) in enumerate(copies):
        copy = pltpu.make_async_copy(src, dst, sems.at[k])
        copy.start()
        started.append(copy)
    for copy in started:
        copy.wait()


def together_of(nz):
    return 2 if nz // SUB % 4 == 0 else 1


def late_groups(nz):
    groups, together = nz // SUB, together_of(nz)
    return {0, *range(groups - 1 - together * (together - 1), groups, together)}


def padded(nz):
    return nz + SUB if nz % 16 == 0 else nz


def bulk_kernel(dims, counts, step, *refs):
    rows, nx, nz = dims
    first, last = step == 0, step == STEPS - 1
    n_src = 1 + counts[0] if first else rows
    src, refs = refs[:n_src], refs[n_src:]
    halos, refs = refs[: counts[0]], refs[counts[0] :]
    crowding, refs = refs[0], refs[1 + first :]
    py = lax.rem(lax.axis_index("rows"), 2)
    order = [mirrored(j, py, rows) for j in range(rows)]
    pitch = nz + 1
    groups = nz // SUB
    together = together_of(nz)
    span = together * together * SUB
    piece = together * SUB
    blocks = nz // span
    copies = []
    if first:
        outs, (cells, sems) = refs[:rows], refs[rows:]
        landed = preloaded(nz) // piece
        held = face_rows(counts[0], rows)
        fetched = fetched_rows(counts[0], rows)
        planes_of = [src[1 + held[j]] if j in held else cells.at[fetched.index(j)] for j in range(rows)]
        for k in range(landed, nz // piece):
            for n, j in enumerate(fetched):
                at = (slice(None), pl.ds(k * piece, piece), slice(None))
                dst = cells.at[n].at[at]
                copies.append(pltpu.make_async_copy(src[0].at[order[j]].at[at], dst, sems.at[k, n]))
                copies[-1].start()
    elif last:
        done, outs, sems = refs[0], refs[1 : 1 + rows], refs[1 + rows]
    else:
        outs = refs

    if not last:
        zero = jnp.zeros((SUB, 128), jnp.float32)
        for out in outs:
            for x in range(0, nx, SUB):
                out[pl.ds(x * pitch, SUB, stride=pitch), :] = zero
            out[pl.ds(nx * pitch, SUB), :] = zero

    scale = 2.0 * 10.0**-step

    def columns(z, edges):
        shifts = [z + k * together * SUB for k in range(together)]

        def load(k, j, x, shift):
            z = shifts[k]
            if first:
                ref = planes_of[j]
                if shift == 0:
                    return ref[x, pl.ds(z, SUB), :]
                if edges[k] == shift:
                    own = ref[x, pl.ds(z, SUB), :]
                    rolled = pltpu.roll(own, (-shift) % SUB, 0)
                    row = lax.broadcasted_iota(jnp.int32, (SUB, 128), 0)
                    return jnp.where(row == (0 if shift < 0 else SUB - 1), 0.0, rolled)
                return ref[x, pl.ds(z + shift, SUB), :]
            return src[j][pl.ds(x * pitch + 1 + z + shift, SUB), :]

        def load_halo(k, which, x):
            if first:
                return halos[which][x, pl.ds(shifts[k], SUB), :]
            return halos[which][pl.ds(x * pitch + 1 + shifts[k], SUB), :]

        def plane(x):
            planes = [[load(k, j, x, 0) for j in range(rows)] for k in range(together)]
            above = [load_halo(k, 0, x) for k in range(together)]
            below = [load_halo(k, 1, x) if counts[0] > 1 else None for k in range(together)]
            return planes, above, below

        def advance(x, carry, final):
            diag, here, below = carry
            after = None if final else plane(x + 1)
            diags = []
            for k in range(together):
                forward = []
                for j in range(-1, rows):
                    own = below[k] if j < 0 else here[k][j]
                    if final:
                        forward.append(own)
                        continue
                    ahead = after[0][k][j + 1] if j + 1 < rows else after[1][k]
                    forward.append(ahead if own is None else own + ahead)
                for j in range(rows):
                    total = load(k, j, x, -1) + load(k, j, x, 1)
                    total = total + diag[k][j]
                    if forward[j] is not None:
                        total = total + forward[j]
                    cell = here[k][j]
                    c = crowding[order[j], x, pl.ds(shifts[k], SUB), :]
                    value = total + cell * (6.0 - (c * scale) * cell)
                    if last:
                        outs[j][x, pl.ds(shifts[k], SUB), :] = value * 10.0**-STEPS
                    else:
                        outs[j][pl.ds(x * pitch + 1 + shifts[k], SUB), :] = value
                diags.append(forward[1:])
            return None if final else (diags, after[0], after[2])

        planes, above, below = plane(0)
        carry = ([planes[k][1:] + [above[k]] for k in range(together)], planes, below)
        unroll = max(k for k in range(1, 22) if (nx - 1) % k == 0)

        def body(i, carry):
            for k in range(unroll):
                carry = advance(i * unroll + k, carry, False)
            return carry

        carry = lax.fori_loop(0, (nx - 1) // unroll, body, carry)
        advance(nx - 1, carry, True)

    def block(base, part, edges):
        columns(base + part * SUB, edges)

    parts = [(k, part) for k in range(blocks) for part in range(together)]
    if first:
        early = landed
        for k, part in parts:
            base = k * span + part * SUB
            top = base + (together - 1) * piece + SUB
            edges = [0] * together
            if base == 0:
                edges[0] = -1
            if top == nz:
                edges[-1] = 1
            while landed * piece < min(top + 1, nz):
                for n in range(len(fetched)):
                    copies[(landed - early) * len(fetched) + n].wait()
                landed += 1
            block(k * span, part, edges)
    elif last:

        def send(group, j):
            at = (slice(None), pl.ds(pl.multiple_of(group * SUB, SUB), SUB), slice(None))
            return pltpu.make_async_copy(outs[j].at[at], done.at[order[j]].at[at], sems.at[group, j])

        @pl.loop(0, blocks)
        def _(k):
            for part in range(together):
                block(pl.multiple_of(k * span, SUB), part, None)
                for g in range(together):
                    group = k * together * together + part + g * together
                    early = [group != left for left in late_groups(nz)]

                    @pl.when(functools.reduce(jnp.logical_and, early))
                    def _():
                        for j in range(rows):
                            send(group, j).start()

        for group in range(groups):
            if group not in late_groups(nz):
                for j in range(rows):
                    send(group, j).wait()
    else:

        @pl.loop(0, blocks)
        def _(k):
            for part in range(together):
                block(pl.multiple_of(k * span, SUB), part, None)


def patch_kernel(dims, counts, step, *refs):
    rows, nx, nz = dims
    last = step == STEPS - 1
    n_state = rows + 1 if last else rows
    n_x, n_z = counts[1], counts[2]
    refs = refs[n_state:]
    halo_x, halo_z, refs = refs[:n_x], refs[n_x : n_x + n_z], refs[n_x + n_z :]
    state, refs = refs[:n_state], refs[n_state:]
    if last:
        done, cells, sems = state[0], state[1:], refs[0]
    else:
        face_x, face_z = refs[:n_x], refs[n_x:]
    py = lax.rem(lax.axis_index("rows"), 2)
    px = lax.rem(lax.axis_index("cols"), 2)
    pz = lax.rem(lax.axis_index("slabs"), 2)
    pitch = padded(nz) if last else nz + 1
    offset = 0 if last else 1

    if last:
        order = [mirrored(j, py, rows) for j in range(rows)]
        views = [cells[j].reshape(nx * pitch, 128) for j in range(rows)]
    else:
        views = state

    def scaled(values):
        return values * 10.0**-STEPS if last else values

    copies = []

    def send(j, at):
        sem = sems.at[len(copies)]
        copies.append(pltpu.make_async_copy(cells[j].at[at], done.at[order[j]].at[at], sem))
        copies[-1].start()

    def patch_z(which):
        z = near(which, pz, nz)
        for j in range(rows):
            for x in range(0, nx, SUB):
                at = (pl.ds(x * pitch + offset + z, SUB, stride=pitch), slice(None))
                views[j][at] = views[j][at] + scaled(halo_z[which][j, pl.ds(x, SUB), :])

    def patch_x(which):
        x = near(which, px, nx)
        for j in range(rows):
            for z in range(0, nz, SUB):
                at = (pl.ds(x * pitch + offset + z, SUB), slice(None))
                value = views[j][at] + scaled(halo_x[which][j, pl.ds(z, SUB), :])
                views[j][at] = value
                if not last:
                    face_x[which][j, pl.ds(z, SUB), :] = value

    if last:
        for group in sorted(late_groups(nz) - {0, nz // SUB - 1}):
            for j in range(rows):
                send(j, (pl.ds(1, nx - 2), pl.ds(group * SUB, SUB), slice(None)))
        for which in range(2):
            if which < n_x:
                patch_x(which)
            for j in range(rows):
                send(j, (near(which, px, nx), pl.ds(SUB, nz - 2 * SUB), slice(None)))
        for which in range(2):
            if which < n_z:
                patch_z(which)
            z = pl.multiple_of(near(which, pz, nz // SUB) * SUB, SUB)
            for j in range(rows):
                send(j, (slice(None), pl.ds(z, SUB), slice(None)))
        for copy in copies:
            copy.wait()
        return
    for which in range(n_z):
        patch_z(which)
    for which in range(n_x):
        patch_x(which)
    for which in range(n_z):
        z = near(which, pz, nz)
        for j in range(rows):
            for x in range(0, nx, SUB):
                at = (pl.ds(x * pitch + offset + z, SUB, stride=pitch), slice(None))
                face_z[which][j, pl.ds(x, SUB), :] = views[j][at]


def call(kernel, name, out_shape, args, out_specs=None, in_specs=None, aliases=None, scratch=(), vmem=1):
    return pl.pallas_call(
        kernel,
        name=name,
        out_shape=out_shape,
        in_specs=in_specs or [VMEM_SPEC] * len(args),
        out_specs=out_specs or [VMEM_SPEC] * len(out_shape),
        input_output_aliases=aliases or {},
        scratch_shapes=list(scratch),
        compiler_params=pltpu.CompilerParams(vmem_limit_bytes=vmem * 1024 * 1024),
    )(*args)


def on_device(tracer, crowding):
    rows, nx, nz, species = tracer.shape
    dims = (rows, nx, nz)
    sizes = [lax.axis_size(axis) for axis in ("rows", "cols", "slabs")]
    counts = [len(matchings(size)) for size in sizes]
    pitch_rows = -(-(nx * (nz + 1) + SUB) // 32) * 32
    f32 = jnp.float32
    padded_row = pltpu.VMEM((nx, padded(nz), species), f32)
    state_row = pltpu.VMEM((pitch_rows, species), f32)
    x_face = pltpu.VMEM((rows, nz, species), f32)
    z_face = pltpu.VMEM((rows, nx, species), f32)

    thin = [(nx, nz, 1, species)] * counts[0] + [(rows, nz, 1, species)] * counts[1]
    thin += [(rows, nx, 1, species)] * counts[2]
    fetched = len(fetched_rows(counts[0], rows))
    thin += [(fetched, nx, nz, 1, species)]
    packed = call(
        functools.partial(pack_kernel, dims, counts),
        "pack",
        [pltpu.VMEM(shape, f32) for shape in thin],
        (pltpu.with_memory_space_constraint(tracer.reshape(rows, nx, nz, 1, species), pltpu.HBM),),
        in_specs=[HBM_SPEC],
        scratch=[pltpu.SemaphoreType.DMA((rows * (1 + counts[1] + counts[2]),))],
    )
    packed = [face.reshape(*face.shape[:-2], species) for face in packed]
    *packed, cells = packed
    y_faces, packed = packed[: counts[0]], packed[counts[0] :]
    x_faces, z_faces = packed[: counts[1]], packed[counts[1] :]
    state = [tracer]
    for step in range(STEPS):
        last = step == STEPS - 1
        y_halos = [swap(face, "rows", k, sizes[0]) for k, face in enumerate(y_faces)]
        x_halos = [swap(face, "cols", k, sizes[1]) for k, face in enumerate(x_faces)]
        z_halos = [swap(face, "slabs", k, sizes[2]) for k, face in enumerate(z_faces)]
        kernel = functools.partial(bulk_kernel, dims, counts, step)
        args = (*state, *y_halos, crowding)
        if step == 0:
            args = (pltpu.with_memory_space_constraint(tracer, pltpu.HBM), *y_faces, *args[1:], cells)
            state = call(
                kernel,
                "bulk0",
                [state_row] * rows + [pltpu.VMEM(cells.shape, f32)],
                args,
                in_specs=[HBM_SPEC] + [VMEM_SPEC] * (len(args) - 1),
                aliases={len(args) - 1: rows},
                scratch=[pltpu.SemaphoreType.DMA((nz // SUB, fetched))],
            )[:rows]
        elif last:
            state = call(
                kernel,
                "bulk_last",
                [pltpu.HBM(tracer.shape, f32)] + [padded_row] * rows,
                args,
                out_specs=[HBM_SPEC] + [VMEM_SPEC] * rows,
                scratch=[pltpu.SemaphoreType.DMA((nz // SUB, rows))],
            )
        else:
            state = call(kernel, f"bulk{step}", [state_row] * rows, args)
        kernel = functools.partial(patch_kernel, dims, counts, step)
        args = (*state, *x_halos, *z_halos)
        aliases = {k: k for k in range(len(state))}
        if last:
            specs = [HBM_SPEC] + [VMEM_SPEC] * rows
            return call(
                kernel,
                "patch_last",
                [pltpu.HBM(tracer.shape, f32)] + [padded_row] * rows,
                args,
                in_specs=specs + [VMEM_SPEC] * (len(args) - len(specs)),
                out_specs=specs,
                aliases=aliases,
                scratch=[pltpu.SemaphoreType.DMA(((2 + len(late_groups(nz))) * rows,))],
            )[0]
        out_shape = [state_row] * rows + [x_face] * counts[1] + [z_face] * counts[2]
        patched = call(kernel, f"patch{step}", out_shape, args, aliases=aliases)
        state = patched[:rows]
        y_faces = [state[rows - 1 if k == 0 else 0] for k in range(counts[0])]
        x_faces = patched[rows : rows + counts[1]]
        z_faces = patched[rows + counts[1] :]


def solution(mesh):
    placed = (P("rows", "cols", "slabs", None), P("rows", "cols", "slabs", None))
    return jax.shard_map(
        on_device,
        mesh=mesh,
        in_specs=placed,
        out_specs=P("rows", "cols", "slabs", None),
        check_vma=False,
    )
```

```python
import functools

import jax
import jax.numpy as jnp
from jax import lax
from jax.experimental import pallas as pl
from jax.experimental.pallas import tpu as pltpu
from jax.sharding import PartitionSpec as P

STEPS = 4
SUB = 8
VMEM_SPEC = pl.BlockSpec(memory_space=pltpu.VMEM)
HBM_SPEC = pl.BlockSpec(memory_space=pltpu.HBM)


def matchings(count):
    swaps = []
    for first in (0, 1):
        pairs = [(i, i + 1) for i in range(first, count - 1, 2)]
        if pairs:
            swaps.append(pairs + [(b, a) for a, b in pairs])
    return swaps


def swap(face, axis, which, count):
    with jax.named_scope(f"swap_{axis}_{which}"):
        return lax.ppermute(face, axis, matchings(count)[which])


def near(which, parity, size):
    high = parity == which
    return jnp.where(high, size - 1, 0)


def mirrored(j, parity, rows):
    return jnp.where(parity == 0, j, rows - 1 - j)


def face_rows(n_y, rows):
    return {rows - 1 if which == 0 else 0: which for which in range(n_y)}


def fetched_rows(n_y, rows):
    return [j for j in range(rows) if j not in face_rows(n_y, rows)]


def preloaded(nz):
    return min(together_of(nz) * 2 * SUB, nz)


def pack_kernel(dims, counts, tracer, *refs):
    rows, nx, nz = dims
    n_y, n_x, n_z = counts
    faces, (cells, sems) = refs[: sum(counts)], refs[sum(counts) :]
    y_faces, x_faces, z_faces = faces[:n_y], faces[n_y : n_y + n_x], faces[n_y + n_x :]
    py = lax.rem(lax.axis_index("rows"), 2)
    px = lax.rem(lax.axis_index("cols"), 2)
    pz = lax.rem(lax.axis_index("slabs"), 2)
    order = [mirrored(j, py, rows) for j in range(rows)]
    copies = []
    for which in range(n_x):
        for j in range(rows):
            copies.append((tracer.at[order[j], near(which, px, nx)], x_faces[which].at[j]))
    for which in range(n_z):
        for j in range(rows):
            copies.append((tracer.at[order[j], :, near(which, pz, nz)], z_faces[which].at[j]))
    for which in range(n_y):
        copies.append((tracer.at[order[rows - 1 if which == 0 else 0]], y_faces[which]))
    ahead = pl.ds(0, preloaded(nz))
    for n, j in enumerate(fetched_rows(n_y, rows)):
        copies.append((tracer.at[order[j], :, ahead], cells.at[n, :, ahead]))
    started = []
    for k, (src, dst) in enumerate(copies):
        copy = pltpu.make_async_copy(src, dst, sems.at[k])
        copy.start()
        started.append(copy)
    for copy in started:
        copy.wait()


def together_of(nz):
    return 2 if nz // SUB % 4 == 0 else 1


def late_groups(nz):
    groups, together = nz // SUB, together_of(nz)
    return {0, *range(groups - 1 - together * (together - 1), groups, together)}


def padded(nz):
    return nz + SUB if nz % 16 == 0 else nz


def bulk_kernel(dims, counts, step, *refs):
    rows, nx, nz = dims
    first, last = step == 0, step == STEPS - 1
    n_src = 1 + counts[0] if first else rows
    src, refs = refs[:n_src], refs[n_src:]
    halos, refs = refs[: counts[0]], refs[counts[0] :]
    crowding, refs = refs[0], refs[1 + first :]
    py = lax.rem(lax.axis_index("rows"), 2)
    order = [mirrored(j, py, rows) for j in range(rows)]
    pitch = nz + 1
    groups = nz // SUB
    together = together_of(nz)
    span = together * together * SUB
    piece = together * SUB
    blocks = nz // span
    copies = []
    if first:
        outs, (cells, sems) = refs[:rows], refs[rows:]
        landed = preloaded(nz) // SUB
        held = face_rows(counts[0], rows)
        fetched = fetched_rows(counts[0], rows)
        planes_of = [src[1 + held[j]] if j in held else cells.at[fetched.index(j)] for j in range(rows)]
        for k in range(landed, nz // SUB):
            for n, j in enumerate(fetched):
                at = (slice(None), pl.ds(k * SUB, SUB), slice(None))
                dst = cells.at[n].at[at]
                copies.append(pltpu.make_async_copy(src[0].at[order[j]].at[at], dst, sems.at[k, n]))
                copies[-1].start()
    elif last:
        done, outs, sems = refs[0], refs[1 : 1 + rows], refs[1 + rows]
    else:
        outs = refs

    if not last:
        zero = jnp.zeros((SUB, 128), jnp.float32)
        for out in outs:
            for x in range(0, nx, SUB):
                out[pl.ds(x * pitch, SUB, stride=pitch), :] = zero
            out[pl.ds(nx * pitch, SUB), :] = zero

    scale = 2.0 * 10.0**-step

    def columns(z, edges):
        shifts = [z + k * together * SUB for k in range(together)]

        def load(k, j, x, shift):
            z = shifts[k]
            if first:
                ref = planes_of[j]
                if shift == 0:
                    return ref[x, pl.ds(z, SUB), :]
                if edges[k] == shift:
                    own = ref[x, pl.ds(z, SUB), :]
                    rolled = pltpu.roll(own, (-shift) % SUB, 0)
                    row = lax.broadcasted_iota(jnp.int32, (SUB, 128), 0)
                    return jnp.where(row == (0 if shift < 0 else SUB - 1), 0.0, rolled)
                return ref[x, pl.ds(z + shift, SUB), :]
            return src[j][pl.ds(x * pitch + 1 + z + shift, SUB), :]

        def load_halo(k, which, x):
            if first:
                return halos[which][x, pl.ds(shifts[k], SUB), :]
            return halos[which][pl.ds(x * pitch + 1 + shifts[k], SUB), :]

        def plane(x):
            planes = [[load(k, j, x, 0) for j in range(rows)] for k in range(together)]
            above = [load_halo(k, 0, x) for k in range(together)]
            below = [load_halo(k, 1, x) if counts[0] > 1 else None for k in range(together)]
            return planes, above, below

        def advance(x, carry, final):
            diag, here, below = carry
            after = None if final else plane(x + 1)
            diags = []
            for k in range(together):
                forward = []
                for j in range(-1, rows):
                    own = below[k] if j < 0 else here[k][j]
                    if final:
                        forward.append(own)
                        continue
                    ahead = after[0][k][j + 1] if j + 1 < rows else after[1][k]
                    forward.append(ahead if own is None else own + ahead)
                for j in range(rows):
                    total = load(k, j, x, -1) + load(k, j, x, 1)
                    total = total + diag[k][j]
                    if forward[j] is not None:
                        total = total + forward[j]
                    cell = here[k][j]
                    c = crowding[order[j], x, pl.ds(shifts[k], SUB), :]
                    value = total + cell * (6.0 - (c * scale) * cell)
                    if last:
                        outs[j][x, pl.ds(shifts[k], SUB), :] = value * 10.0**-STEPS
                    else:
                        outs[j][pl.ds(x * pitch + 1 + shifts[k], SUB), :] = value
                diags.append(forward[1:])
            return None if final else (diags, after[0], after[2])

        planes, above, below = plane(0)
        carry = ([planes[k][1:] + [above[k]] for k in range(together)], planes, below)
        unroll = max(k for k in range(1, 22) if (nx - 1) % k == 0)

        def body(i, carry):
            for k in range(unroll):
                carry = advance(i * unroll + k, carry, False)
            return carry

        carry = lax.fori_loop(0, (nx - 1) // unroll, body, carry)
        advance(nx - 1, carry, True)

    def block(base, part, edges):
        columns(base + part * SUB, edges)

    parts = [(k, part) for k in range(blocks) for part in range(together)]
    if first:
        early = landed
        for k, part in parts:
            base = k * span + part * SUB
            top = base + (together - 1) * piece + SUB
            edges = [0] * together
            if base == 0:
                edges[0] = -1
            if top == nz:
                edges[-1] = 1
            while landed * SUB < min(top + 1, nz):
                for n in range(len(fetched)):
                    copies[(landed - early) * len(fetched) + n].wait()
                landed += 1
            block(k * span, part, edges)
    elif last:

        def send(group, j):
            at = (slice(None), pl.ds(pl.multiple_of(group * SUB, SUB), SUB), slice(None))
            return pltpu.make_async_copy(outs[j].at[at], done.at[order[j]].at[at], sems.at[group, j])

        @pl.loop(0, blocks)
        def _(k):
            for part in range(together):
                block(pl.multiple_of(k * span, SUB), part, None)
                for g in range(together):
                    group = k * together * together + part + g * together
                    early = [group != left for left in late_groups(nz)]

                    @pl.when(functools.reduce(jnp.logical_and, early))
                    def _():
                        for j in range(rows):
                            send(group, j).start()

        for group in range(groups):
            if group not in late_groups(nz):
                for j in range(rows):
                    send(group, j).wait()
    else:

        @pl.loop(0, blocks)
        def _(k):
            for part in range(together):
                block(pl.multiple_of(k * span, SUB), part, None)


def patch_kernel(dims, counts, step, *refs):
    rows, nx, nz = dims
    last = step == STEPS - 1
    n_state = rows + 1 if last else rows
    n_x, n_z = counts[1], counts[2]
    refs = refs[n_state:]
    halo_x, halo_z, refs = refs[:n_x], refs[n_x : n_x + n_z], refs[n_x + n_z :]
    state, refs = refs[:n_state], refs[n_state:]
    if last:
        done, cells, sems = state[0], state[1:], refs[0]
    else:
        face_x, face_z = refs[:n_x], refs[n_x:]
    py = lax.rem(lax.axis_index("rows"), 2)
    px = lax.rem(lax.axis_index("cols"), 2)
    pz = lax.rem(lax.axis_index("slabs"), 2)
    pitch = padded(nz) if last else nz + 1
    offset = 0 if last else 1

    if last:
        order = [mirrored(j, py, rows) for j in range(rows)]
        views = [cells[j].reshape(nx * pitch, 128) for j in range(rows)]
    else:
        views = state

    def scaled(values):
        return values * 10.0**-STEPS if last else values

    copies = []

    def send(j, at):
        sem = sems.at[len(copies)]
        copies.append(pltpu.make_async_copy(cells[j].at[at], done.at[order[j]].at[at], sem))
        copies[-1].start()

    def patch_z(which):
        z = near(which, pz, nz)
        for j in range(rows):
            for x in range(0, nx, SUB):
                at = (pl.ds(x * pitch + offset + z, SUB, stride=pitch), slice(None))
                views[j][at] = views[j][at] + scaled(halo_z[which][j, pl.ds(x, SUB), :])

    def patch_x(which):
        x = near(which, px, nx)
        for j in range(rows):
            for z in range(0, nz, SUB):
                at = (pl.ds(x * pitch + offset + z, SUB), slice(None))
                value = views[j][at] + scaled(halo_x[which][j, pl.ds(z, SUB), :])
                views[j][at] = value
                if not last:
                    face_x[which][j, pl.ds(z, SUB), :] = value

    if last:
        for group in sorted(late_groups(nz) - {0, nz // SUB - 1}):
            for j in range(rows):
                send(j, (pl.ds(1, nx - 2), pl.ds(group * SUB, SUB), slice(None)))
        for which in range(2):
            if which < n_x:
                patch_x(which)
            for j in range(rows):
                send(j, (near(which, px, nx), pl.ds(SUB, nz - 2 * SUB), slice(None)))
        for which in range(2):
            if which < n_z:
                patch_z(which)
            z = pl.multiple_of(near(which, pz, nz // SUB) * SUB, SUB)
            for j in range(rows):
                send(j, (slice(None), pl.ds(z, SUB), slice(None)))
        for copy in copies:
            copy.wait()
        return
    for which in range(n_z):
        patch_z(which)
    for which in range(n_x):
        patch_x(which)
    for which in range(n_z):
        z = near(which, pz, nz)
        for j in range(rows):
            for x in range(0, nx, SUB):
                at = (pl.ds(x * pitch + offset + z, SUB, stride=pitch), slice(None))
                face_z[which][j, pl.ds(x, SUB), :] = views[j][at]


def call(kernel, name, out_shape, args, out_specs=None, in_specs=None, aliases=None, scratch=(), vmem=1):
    return pl.pallas_call(
        kernel,
        name=name,
        out_shape=out_shape,
        in_specs=in_specs or [VMEM_SPEC] * len(args),
        out_specs=out_specs or [VMEM_SPEC] * len(out_shape),
        input_output_aliases=aliases or {},
        scratch_shapes=list(scratch),
        compiler_params=pltpu.CompilerParams(vmem_limit_bytes=vmem * 1024 * 1024),
    )(*args)


def on_device(tracer, crowding):
    rows, nx, nz, species = tracer.shape
    dims = (rows, nx, nz)
    sizes = [lax.axis_size(axis) for axis in ("rows", "cols", "slabs")]
    counts = [len(matchings(size)) for size in sizes]
    pitch_rows = -(-(nx * (nz + 1) + SUB) // 32) * 32
    f32 = jnp.float32
    padded_row = pltpu.VMEM((nx, padded(nz), species), f32)
    state_row = pltpu.VMEM((pitch_rows, species), f32)
    x_face = pltpu.VMEM((rows, nz, species), f32)
    z_face = pltpu.VMEM((rows, nx, species), f32)

    thin = [(nx, nz, 1, species)] * counts[0] + [(rows, nz, 1, species)] * counts[1]
    thin += [(rows, nx, 1, species)] * counts[2]
    fetched = len(fetched_rows(counts[0], rows))
    thin += [(fetched, nx, nz, 1, species)]
    packed = call(
        functools.partial(pack_kernel, dims, counts),
        "pack",
        [pltpu.VMEM(shape, f32) for shape in thin],
        (pltpu.with_memory_space_constraint(tracer.reshape(rows, nx, nz, 1, species), pltpu.HBM),),
        in_specs=[HBM_SPEC],
        scratch=[pltpu.SemaphoreType.DMA((rows * (1 + counts[1] + counts[2]),))],
    )
    packed = [face.reshape(*face.shape[:-2], species) for face in packed]
    *packed, cells = packed
    y_faces, packed = packed[: counts[0]], packed[counts[0] :]
    x_faces, z_faces = packed[: counts[1]], packed[counts[1] :]
    state = [tracer]
    for step in range(STEPS):
        last = step == STEPS - 1
        y_halos = [swap(face, "rows", k, sizes[0]) for k, face in enumerate(y_faces)]
        x_halos = [swap(face, "cols", k, sizes[1]) for k, face in enumerate(x_faces)]
        z_halos = [swap(face, "slabs", k, sizes[2]) for k, face in enumerate(z_faces)]
        kernel = functools.partial(bulk_kernel, dims, counts, step)
        args = (*state, *y_halos, crowding)
        if step == 0:
            args = (pltpu.with_memory_space_constraint(tracer, pltpu.HBM), *y_faces, *args[1:], cells)
            state = call(
                kernel,
                "bulk0",
                [state_row] * rows + [pltpu.VMEM(cells.shape, f32)],
                args,
                in_specs=[HBM_SPEC] + [VMEM_SPEC] * (len(args) - 1),
                aliases={len(args) - 1: rows},
                scratch=[pltpu.SemaphoreType.DMA((nz // SUB, fetched))],
            )[:rows]
        elif last:
            state = call(
                kernel,
                "bulk_last",
                [pltpu.HBM(tracer.shape, f32)] + [padded_row] * rows,
                args,
                out_specs=[HBM_SPEC] + [VMEM_SPEC] * rows,
                scratch=[pltpu.SemaphoreType.DMA((nz // SUB, rows))],
            )
        else:
            state = call(kernel, f"bulk{step}", [state_row] * rows, args)
        kernel = functools.partial(patch_kernel, dims, counts, step)
        args = (*state, *x_halos, *z_halos)
        aliases = {k: k for k in range(len(state))}
        if last:
            specs = [HBM_SPEC] + [VMEM_SPEC] * rows
            return call(
                kernel,
                "patch_last",
                [pltpu.HBM(tracer.shape, f32)] + [padded_row] * rows,
                args,
                in_specs=specs + [VMEM_SPEC] * (len(args) - len(specs)),
                out_specs=specs,
                aliases=aliases,
                scratch=[pltpu.SemaphoreType.DMA(((2 + len(late_groups(nz))) * rows,))],
            )[0]
        out_shape = [state_row] * rows + [x_face] * counts[1] + [z_face] * counts[2]
        patched = call(kernel, f"patch{step}", out_shape, args, aliases=aliases)
        state = patched[:rows]
        y_faces = [state[rows - 1 if k == 0 else 0] for k in range(counts[0])]
        x_faces = patched[rows : rows + counts[1]]
        z_faces = patched[rows + counts[1] :]


def solution(mesh):
    placed = (P("rows", "cols", "slabs", None), P("rows", "cols", "slabs", None))
    return jax.shard_map(
        on_device,
        mesh=mesh,
        in_specs=placed,
        out_specs=P("rows", "cols", "slabs", None),
        check_vma=False,
    )
```
